32 devices in a mesh: tp: 4 (over x, core), fsdp: 8 (over z, y).
Axes of the slice: x: 2, y: 2, z: 4, core: 2. Of those that a mesh axis runs over, the one named last changes fastest.
Arguments:
- sectioned: bfloat16 [64, 256, 26624], P('fsdp', None, 'tp'), as said below
- loader_owner: int32 [64], replicated, may hold values from 0 to 7, as said below
- slab_order: int32 [64], replicated, may hold values from 0 to 7, as said below
Outputs:
- dequant: bfloat16 [16384, 26624], P(('tp', 'fsdp'))
- scale_codes: float32 [26624, 256], P(('tp', 'fsdp'))
- group_max: float32 [26624], P(('tp', 'fsdp'))
The draws below stay inside these ranges and needn't reach their ends.
Inputs may be any that keep to these rules, and one draw needn't show every extreme that they name: `loader_owner`: slab s holds rows s * 256 to (s + 1) * 256 - 1; for each f, the 8 slabs s with (s // 2) % 8 == f have 8 distinct owners. `slab_order`: the slabs of one owner have distinct orders. `sectioned`: entries are finite.
All inputs are finite; a program needn't handle non-finite values. Where the reference program divides by a largest or mean magnitude, that divisor is 1e-20 or more.
Results may differ from the reference program's by a relative error of at most 0.0015.
Values may be sent and summed in bfloat16 or wider, within the bound.
A program may use at most 256 MiB of HBM per device.

```python
import jax
import jax.numpy as jnp
from jax import lax

D = 16384
FFW = 26624
OWNERS = 8
SLABS = 64
SR = 256
SPB = 2
N_TP = 4
N_FSDP = 8


def loader_layout(key):
    first = jax.random.fold_in(key, 11)
    second = jax.random.fold_in(key, 12)
    rng = jnp.arange(N_FSDP)
    owners = jax.vmap(lambda f: jax.random.permutation(jax.random.fold_in(first, f), N_FSDP))(rng)
    slots = jax.vmap(lambda o: jax.random.permutation(jax.random.fold_in(second, o), N_FSDP))(rng)
    slab = jnp.arange(SLABS)
    block = slab // SPB
    target = block % N_FSDP
    place = block // N_FSDP * SPB + slab % SPB
    owner = owners[target, place]
    order = slots[owner, target]
    return (owner.astype(jnp.int32), order.astype(jnp.int32))


def draw_loader_owner(key, part):
    return loader_layout(key)[0]


def draw_slab_order(key, part):
    return loader_layout(key)[1]


def draw_sectioned(key, part):
    owner, order = loader_layout(key)
    slot = owner * N_FSDP + order
    slab_at = jnp.zeros((SLABS,), jnp.int32).at[slot].set(jnp.arange(SLABS, dtype=jnp.int32))
    owner_of_slot = (jnp.arange(SLABS) // N_FSDP).astype(jnp.float32)
    block_pos = (slab_at // SPB).astype(jnp.float32)
    level = jnp.exp(jnp.log(3.0) * (owner_of_slot / max(N_FSDP - 1, 1) + block_pos / max(N_TP * N_FSDP - 1, 1)))
    noise_key = jax.random.fold_in(key, 13)
    values = jax.random.normal(noise_key, (SLABS, SR, FFW), jnp.float32) * 0.5
    return (values * level[:, None, None]).astype(jnp.bfloat16)


def setup_inputs(seed: int = 0) -> dict:
    seeds = jax.random.split(jax.random.key(seed), 4)
    sectioned = draw_sectioned(jax.random.fold_in(seeds[3], 71), 0)
    loader_owner = draw_loader_owner(jax.random.fold_in(seeds[3], 71), 0)
    slab_order = draw_slab_order(jax.random.fold_in(seeds[3], 71), 0)
    return {"sectioned": sectioned, "loader_owner": loader_owner, "slab_order": slab_order}


LEVELS = [-1.0, -0.6961928009986877, -0.5250730514526367, -0.39491748809814453,
          -0.28444138169288635, -0.18477343022823334, -0.09105003625154495, 0.0,
          0.07958029955625534, 0.16093020141124725, 0.24611230194568634, 0.33791524171829224,
          0.44070982933044434, 0.5626170039176941, 0.7229568362236023, 1.0]
MIDPOINTS = [(LEVELS[k] + LEVELS[k + 1]) / 2.0 for k in range(15)]
STEPSIZES = [LEVELS[k + 1] - LEVELS[k] for k in range(15)]
EPS = 1e-6


def hard_code(block):
    values = block.astype(jnp.float32)
    shape = values.shape
    grouped = values.reshape(shape[:-1] + (shape[-1] // 64, 64))
    absmax = jnp.max(jnp.abs(grouped), axis=-1)
    spread = jnp.repeat(absmax, 64, axis=-1)
    ratio = values / (spread + EPS)
    level = jnp.full(shape, LEVELS[0], jnp.float32)
    for middle, stepsize in zip(MIDPOINTS, STEPSIZES):
        level = level + jnp.where(ratio > middle, stepsize, 0.0).astype(jnp.float32)
    coded = (spread * level).astype(jnp.bfloat16)
    return coded, absmax


def reference(sectioned, loader_owner, slab_order):
    slot = (loader_owner * OWNERS + slab_order).astype(jnp.int32)
    weight = jnp.take(sectioned, slot, axis=0).reshape(64, D // 64, FFW)
    coded, absmax = lax.map(hard_code, weight)
    dequant = coded.reshape(D, FFW)
    absmax = absmax.reshape(D, FFW // 64)
    offset = jnp.sum(absmax) / float(D * FFW // 64)
    centred = absmax.reshape(-1, 256) - offset
    group_max = jnp.max(jnp.abs(centred), axis=1)
    scale_codes = centred / (group_max[:, None] + EPS)
    return dequant, scale_codes, group_max
```

```python
import functools
import math

import jax
import jax.numpy as jnp
import numpy as np
from jax import lax
from jax.experimental import pallas as pl
from jax.experimental.pallas import tpu as pltpu
from jax.sharding import PartitionSpec as P

LEVELS = [
    -1.0,
    -0.6961928009986877,
    -0.5250730514526367,
    -0.39491748809814453,
    -0.28444138169288635,
    -0.18477343022823334,
    -0.09105003625154495,
    0.0,
    0.07958029955625534,
    0.16093020141124725,
    0.24611230194568634,
    0.33791524171829224,
    0.44070982933044434,
    0.5626170039176941,
    0.7229568362236023,
    1.0,
]
MIDPOINTS = [(LEVELS[k] + LEVELS[k + 1]) / 2.0 for k in range(15)]
STEPSIZES = [LEVELS[k + 1] - LEVELS[k] for k in range(15)]
EPS = 1e-06
LANES = 128
BLOCK = 64
MESH = pl.DeviceIdType.MESH


def reached_levels():
    total = np.float32(LEVELS[0])
    reached = [float(total)]
    for step in STEPSIZES:
        total = np.float32(total + np.float32(step))
        reached.append(float(total))
    return reached


REACHED = reached_levels()


def code_tile(w):
    lane = lax.broadcasted_iota(jnp.int32, w.shape, 1)
    top = jnp.abs(w)
    low = lane < BLOCK
    first = jnp.broadcast_to(jnp.max(jnp.where(low, top, 0.0), axis=1, keepdims=True), w.shape)
    second = jnp.broadcast_to(jnp.max(jnp.where(low, 0.0, top), axis=1, keepdims=True), w.shape)
    spread = jnp.where(lane < BLOCK, first, second)
    ratio = w / (spread + EPS)
    level = jnp.full(w.shape, REACHED[0], jnp.float32)
    for middle, value in zip(MIDPOINTS, REACHED[1:]):
        level = jnp.where(ratio > middle, value, level)
    return spread * level, first, second


def exchange(
    sizes, loader_owner, slab_order, sectioned, out, kept, scales, peaks, sums, arrive, ld, pick, snd, own, stage,
    coded, tops, mine, ours, got, met, slots, origin, ls, s1, r1, s2, r2, sa, ra, sm, rm, so, ro,
):
    owners, tp, slab_rows, rows, pieces, per_block, columns, ahead, loads, sends, codes = sizes
    t = lax.axis_index("tp")
    f = lax.axis_index("fsdp")
    width = columns // pieces
    tiles = width // LANES
    chunks = slab_rows // rows * pieces

    def row_span(c):
        return pl.ds(pl.multiple_of(c // pieces * rows, rows), rows)

    def column_span(c):
        return pl.ds(pl.multiple_of(lax.rem(c, pieces) * width, LANES), width)

    def load(c):
        slot = lax.rem(c, loads)
        return pltpu.make_async_copy(sectioned.at[:, row_span(c), column_span(c)], ld.at[slot], ls.at[slot])

    for c in range(min(loads, chunks)):
        load(c).start()

    barrier = pltpu.get_barrier_semaphore()
    for d in range(1, owners):
        pl.semaphore_signal(barrier, inc=1, device_id={"fsdp": lax.rem(f + d, owners)}, device_id_type=MESH)
    for e in range(1, tp):
        pl.semaphore_signal(barrier, inc=1, device_id={"tp": lax.rem(t + e, tp)}, device_id_type=MESH)

    def find_slot(d, _):
        to = lax.rem(f + d, owners)

        def look(p, found):
            s = (p // per_block * owners + to) * per_block + lax.rem(p, per_block)
            return jnp.where(loader_owner[s] == f, slab_order[s], found)

        slots[d] = lax.fori_loop(0, owners, look, 0)
        origin[d] = loader_owner[(d // per_block * owners + f) * per_block + lax.rem(d, per_block)]
        return 0

    lax.fori_loop(0, owners, find_slot, 0)
    mine[...] = jnp.zeros_like(mine)
    peaks[...] = jnp.zeros_like(peaks)
    tops[...] = jnp.zeros_like(tops)
    pl.semaphore_wait(barrier, owners - 1 + tp - 1)

    def first_hop(c, d):
        slot = lax.rem(c, sends)
        return pltpu.make_async_remote_copy(
            src_ref=snd.at[slot, d - 1],
            dst_ref=arrive.at[c, f],
            send_sem=s1.at[slot],
            recv_sem=r1.at[c],
            device_id={"fsdp": lax.rem(f + d, owners)},
            device_id_type=MESH,
        )

    def first_sent(slot):
        whole = snd.at[slot]
        pltpu.make_async_copy(whole, whole, s1.at[slot]).wait()

    def first_landed(c):
        whole = arrive.at[c, pl.ds(0, owners - 1)]
        pltpu.make_async_copy(whole, whole, r1.at[c]).wait()

    low = lax.broadcasted_iota(jnp.int32, (rows, LANES), 1) < BLOCK

    def push(c):
        load(c).wait()

        @pl.when(c >= sends)
        def _():
            first_sent(lax.rem(c, sends))

        def take(o, _):
            pick[o] = ld[lax.rem(c, loads), o]
            return 0

        lax.fori_loop(0, owners, take, 0)

        @pl.when(c + loads < chunks)
        def _():
            load(c + loads).start()

        def choose(d, _):
            snd[lax.rem(c, sends), d - 1] = pick[slots[d]]
            return 0

        lax.fori_loop(1, owners, choose, 0)
        own[lax.rem(c, sends)] = pick[slots[0]]
        for d in order(owners):
            first_hop(c, d).start()

        def add(o, _):
            w = jnp.abs(pick[o].astype(jnp.float32))
            total = jnp.zeros((rows, LANES), jnp.float32)
            for j in range(tiles):
                top = w[:, j * LANES : (j + 1) * LANES]
                first = jnp.max(jnp.where(low, top, 0.0), axis=1, keepdims=True)
                second = jnp.max(jnp.where(low, 0.0, top), axis=1, keepdims=True)
                total = total + jnp.broadcast_to(first + second, total.shape)
            mine[...] += total
            return 0

        lax.fori_loop(0, owners, add, 0)

    def second_hop(c, e):
        slot = lax.rem(c, codes)
        return pltpu.make_async_remote_copy(
            src_ref=coded.at[slot, e - 1],
            dst_ref=out.at[e - 1, :, row_span(c), column_span(c)],
            send_sem=s2.at[slot],
            recv_sem=r2.at[c],
            device_id={"tp": lax.rem(t + e, tp)},
            device_id_type=MESH,
        )

    def second_sent(slot):
        whole = coded.at[slot]
        pltpu.make_async_copy(whole, whole, s2.at[slot]).wait()

    def second_landed(c):
        whole = coded.at[0]
        pltpu.make_async_copy(whole, whole, r2.at[c]).wait()

    def top_hop(r, e):
        span = pl.ds(pl.multiple_of(r * rows, rows), rows)
        return pltpu.make_async_remote_copy(
            src_ref=tops.at[e - 1, :, span],
            dst_ref=scales.at[e - 1, :, span],
            send_sem=sa.at[r],
            recv_sem=ra.at[r],
            device_id={"tp": lax.rem(t + e, tp)},
            device_id_type=MESH,
        )

    def top_done(r, sem):
        span = pl.ds(pl.multiple_of(r * rows, rows), rows)
        whole = tops.at[:, :, span]
        pltpu.make_async_copy(whole, whole, sem.at[r]).wait()

    def code(c, e):
        lane = lax.broadcasted_iota(jnp.int32, (rows, LANES), 1)
        to = lax.rem(t + e, tp)
        start = lax.rem(c, pieces) * (2 * tiles)

        def place(k, _):
            w = stage[origin[to * per_block + k]].astype(jnp.float32)
            if e < tp:
                held = tops[e - 1, k, row_span(c), :]
            else:
                held = peaks[k, row_span(c), :]
            made = []
            for j in range(tiles):
                value, first, second = code_tile(w[:, j * LANES : (j + 1) * LANES])
                made.append(value.astype(jnp.bfloat16))
                index = start + 2 * j
                held = jnp.where(lane == index, first, jnp.where(lane == index + 1, second, held))
            made = jnp.concatenate(made, axis=1)
            if e < tp:
                coded[lax.rem(c, codes), e - 1, k] = made
                tops[e - 1, k, row_span(c), :] = held
            else:
                kept[k, row_span(c), column_span(c)] = made
                peaks[k, row_span(c), :] = held
            return 0

        lax.fori_loop(0, per_block, place, 0)

    def sum_hop(d):
        return pltpu.make_async_remote_copy(
            src_ref=mine,
            dst_ref=got.at[d],
            send_sem=sm.at[d],
            recv_sem=rm.at[d],
            device_id={"fsdp": lax.rem(f + d, owners)},
            device_id_type=MESH,
        )

    def sum_turn(e):
        return pltpu.make_async_remote_copy(
            src_ref=ours,
            dst_ref=met.at[e],
            send_sem=so.at[e],
            recv_sem=ro.at[e],
            device_id={"tp": lax.rem(t + e, tp)},
            device_id_type=MESH,
        )

    def start_sums():
        for d in range(1, owners):
            sum_hop(d).start()

    def prime(c, _):
        push(c)
        return 0

    lax.fori_loop(0, ahead, prime, 0)
    if ahead == chunks:
        start_sums()

    def chunk(c, _):
        @pl.when(c + ahead < chunks)
        def _():
            push(c + ahead)

        if ahead < chunks:

            @pl.when(c + ahead == chunks - 1)
            def _():
                start_sums()

        first_landed(c)

        def take(d, _):
            o = lax.rem(f + d, owners)
            stage[o] = arrive[c, o]
            return 0

        lax.fori_loop(1, owners, take, 0)
        stage[f] = own[lax.rem(c, sends)]

        @pl.when(c >= codes)
        def _():
            second_sent(lax.rem(c, codes))

        for e in range(1, tp + 1):
            code(c, e)
            if e < tp:
                second_hop(c, e).start()

        @pl.when(lax.rem(c, pieces) == pieces - 1)
        def _():
            for e in range(1, tp):
                top_hop(c // pieces, e).start()

        return 0

    lax.fori_loop(0, chunks, chunk, 0)

    for d in range(1, owners):
        sum_hop(d).wait()
    total = mine[...]
    for d in range(1, owners):
        total = total + got[d]
    ours[...] = total
    for e in range(1, tp):
        sum_turn(e).start()
    for c in range(max(chunks - sends, 0), chunks):
        first_sent(c % sends)
    for c in range(max(chunks - codes, 0), chunks):
        second_sent(c % codes)

    def settle_tops(r, _):
        top_done(r, sa)
        top_done(r, ra)
        return 0

    lax.fori_loop(0, chunks // pieces, settle_tops, 0)

    def finish(c, _):
        second_landed(c)
        return 0

    lax.fori_loop(0, chunks, finish, 0)
    for e in range(1, tp):
        sum_turn(e).wait()
    total = ours[...]
    for e in range(1, tp):
        total = total + met[e]
    sums[...] = total


def order(owners):
    middle = owners // 2
    return sorted(range(1, owners), key=lambda d: (abs(d - middle), d))


def place_out(sizes, coded, kept, scales, peaks, sums, out, codes_out, tops_out, codes, spread, table, sem, sent):
    blocks, entries, count = sizes
    per_block, slab_rows, width = kept.shape
    tp = table.shape[0]
    me = lax.axis_index("tp")
    group = 256
    copies = []
    for e in range(tp):
        t = lax.rem(me + tp - e, tp)
        band = out.at[:, :, pl.ds(pl.multiple_of(t * width, LANES), width)]
        copies.append(pltpu.make_async_copy(coded.at[e - 1] if e else kept, band, sem.at[e]))
        copies[-1].start()
    for e in range(tp):
        table[lax.rem(me + tp - e, tp)] = scales[e - 1] if e else peaks[...]

    step = math.gcd(entries, group)
    period, turns = group // step, entries // step
    height = per_block * slab_rows // period
    lane = lax.broadcasted_iota(jnp.int32, (height, LANES), 1)
    offset = jnp.sum(sums[...], axis=0, keepdims=True) / count

    columns = [None] * (2 * turns)

    def lay(at, value):
        columns[at] = value if columns[at] is None else columns[at] + value

    def emit(j):
        left = columns[2 * j] - offset
        right = columns[2 * j + 1] - offset
        largest = jnp.maximum(jnp.abs(left), jnp.abs(right))
        largest = jnp.broadcast_to(jnp.max(largest, axis=1, keepdims=True), left.shape)
        scale = largest + EPS
        rows = pl.ds(j, height, stride=turns)
        codes[0, rows, :] = left / scale
        codes[1, rows, :] = right / scale
        spread[rows, :] = largest

    done = 0
    for i in range(period):
        for t in range(tp):
            piece = table[t, pl.ds(i, height, stride=period), :]
            at, shift = divmod(i * entries + t * blocks, LANES)
            if shift:
                piece = pltpu.roll(piece, shift, 1)
                lay(at, jnp.where(lane >= shift, piece, 0.0))
                if shift + blocks > LANES:
                    lay(at + 1, jnp.where(lane < shift, piece, 0.0))
            else:
                lay(at, piece)
            filled = (i * entries + (t + 1) * blocks) // group
            while done < filled:
                emit(done)
                done += 1

    row = lax.broadcasted_iota(jnp.int32, (LANES, LANES), 0)
    diagonal = row == lax.broadcasted_iota(jnp.int32, (LANES, LANES), 1)
    total = codes.shape[1]
    for s in range(total // LANES + (total % LANES > 0)):
        size = min(LANES, total - s * LANES)
        part = jnp.where(diagonal[:size], spread[s * LANES : s * LANES + size, :], 0.0)
        tops_out[s : s + 1, :] = jnp.sum(part, axis=0, keepdims=True)
    for h in range(2):
        copies.append(pltpu.make_async_copy(codes.at[h], codes_out.at[:, pl.ds(h * LANES, LANES)], sent.at[h]))
        copies[-1].start()
    for copy in copies:
        copy.wait()


def per_device(sectioned, loader_owner, slab_order):
    owners = lax.axis_size("fsdp")
    tp = lax.axis_size("tp")
    slots, slab_rows, columns = sectioned.shape
    slab_count = loader_owner.shape[0]
    per_block = owners // tp
    rows = min(16, slab_rows)
    groups = columns // LANES
    pieces = next(p for p in (4, 2, 1) if groups % p == 0)
    width = columns // pieces
    chunks = slab_rows // rows * pieces
    ahead = min(8, chunks)
    loads, sends, codes = 2, min(ahead + 2, chunks), min(3, chunks)
    blocks = columns // BLOCK
    sizes = (owners, tp, slab_rows, rows, pieces, per_block, columns, ahead, loads, sends, codes)
    dma = pltpu.SemaphoreType.DMA
    anywhere = pl.BlockSpec(memory_space=pl.ANY)
    vmem = pl.BlockSpec(memory_space=pltpu.VMEM)
    smem = pl.BlockSpec(memory_space=pltpu.SMEM)
    half, full = jnp.bfloat16, jnp.float32
    buffers = [
        ((chunks, owners, rows, width), half),
        ((loads, owners, rows, width), half),
        ((owners, rows, width), half),
        ((sends, owners - 1, rows, width), half),
        ((sends, rows, width), half),
        ((owners, rows, width), half),
        ((codes, tp - 1, per_block, rows, width), half),
        ((tp - 1, per_block, slab_rows, LANES), full),
        ((rows, LANES), full),
        ((rows, LANES), full),
        ((owners, rows, LANES), full),
        ((tp, rows, LANES), full),
    ]
    held = sum(int(np.prod(shape)) * jnp.dtype(kind).itemsize for shape, kind in buffers)
    coded, kept, scales, peaks, sums = pl.pallas_call(
        functools.partial(exchange, sizes),
        out_shape=(
            pltpu.VMEM((tp - 1, per_block, slab_rows, columns), half),
            pltpu.VMEM((per_block, slab_rows, columns), half),
            pltpu.VMEM((tp - 1, per_block, slab_rows, LANES), full),
            pltpu.VMEM((per_block, slab_rows, LANES), full),
            pltpu.VMEM((rows, LANES), full),
        ),
        in_specs=[smem, smem, anywhere],
        out_specs=(vmem,) * 5,
        scratch_shapes=[pltpu.VMEM(shape, kind) for shape, kind in buffers]
        + [
            pltpu.SMEM((owners,), jnp.int32),
            pltpu.SMEM((owners,), jnp.int32),
            dma((loads,)),
            dma((sends,)),
            dma((chunks,)),
            dma((codes,)),
            dma((chunks,)),
            dma((chunks // pieces,)),
            dma((chunks // pieces,)),
            dma((owners,)),
            dma((owners,)),
            dma((tp,)),
            dma((tp,)),
        ],
        compiler_params=pltpu.CompilerParams(
            collective_id=0, has_side_effects=True, vmem_limit_bytes=held + 3 * 2**19
        ),
        name="exchange",
    )(loader_owner, slab_order, sectioned)
    entries = tp * blocks
    total = per_block * slab_rows * entries // 256
    lines = -(-total // LANES)
    dequant, scale_codes, tops = pl.pallas_call(
        functools.partial(place_out, (blocks, entries, float(slab_count * slab_rows * entries))),
        out_shape=(
            jax.ShapeDtypeStruct((per_block, slab_rows, tp * columns), half),
            jax.ShapeDtypeStruct((total, 2 * LANES), full),
            jax.ShapeDtypeStruct((lines, LANES), full),
        ),
        in_specs=[vmem] * 5,
        out_specs=(anywhere, anywhere, vmem),
        scratch_shapes=[
            pltpu.VMEM((2, total, LANES), full),
            pltpu.VMEM((total, LANES), full),
            pltpu.VMEM((tp, per_block * slab_rows, LANES), full),
            dma((tp,)),
            dma((2,)),
        ],
        compiler_params=pltpu.CompilerParams(vmem_limit_bytes=7 * 2**19),
        name="place_out",
    )(coded, kept, scales.reshape(tp - 1, -1, LANES), peaks.reshape(-1, LANES), sums)
    dequant = dequant.reshape(per_block * slab_rows, tp * columns)
    return (dequant, scale_codes, tops.reshape(-1)[:total])


def solution(mesh):
    return jax.shard_map(
        per_device,
        mesh=mesh,
        in_specs=(P("fsdp", None, "tp"), P(), P()),
        out_specs=(P(("tp", "fsdp"), None), P(("tp", "fsdp"), None), P(("tp", "fsdp"))),
        check_vma=False,
    )
```

```python
import functools
import math

import jax
import jax.numpy as jnp
import numpy as np
from jax import lax
from jax.experimental import pallas as pl
from jax.experimental.pallas import tpu as pltpu
from jax.sharding import PartitionSpec as P

LEVELS = [
    -1.0,
    -0.6961928009986877,
    -0.5250730514526367,
    -0.39491748809814453,
    -0.28444138169288635,
    -0.18477343022823334,
    -0.09105003625154495,
    0.0,
    0.07958029955625534,
    0.16093020141124725,
    0.24611230194568634,
    0.33791524171829224,
    0.44070982933044434,
    0.5626170039176941,
    0.7229568362236023,
    1.0,
]
MIDPOINTS = [(LEVELS[k] + LEVELS[k + 1]) / 2.0 for k in range(15)]
STEPSIZES = [LEVELS[k + 1] - LEVELS[k] for k in range(15)]
EPS = 1e-06
LANES = 128
BLOCK = 64
MESH = pl.DeviceIdType.MESH


def reached_levels():
    total = np.float32(LEVELS[0])
    reached = [float(total)]
    for step in STEPSIZES:
        total = np.float32(total + np.float32(step))
        reached.append(float(total))
    return reached


REACHED = reached_levels()


def code_tile(w):
    lane = lax.broadcasted_iota(jnp.int32, w.shape, 1)
    top = jnp.abs(w)
    low = lane < BLOCK
    first = jnp.broadcast_to(jnp.max(jnp.where(low, top, 0.0), axis=1, keepdims=True), w.shape)
    second = jnp.broadcast_to(jnp.max(jnp.where(low, 0.0, top), axis=1, keepdims=True), w.shape)
    spread = jnp.where(lane < BLOCK, first, second)
    ratio = w / (spread + EPS)
    level = jnp.full(w.shape, REACHED[0], jnp.float32)
    for middle, value in zip(MIDPOINTS, REACHED[1:]):
        level = jnp.where(ratio > middle, value, level)
    return spread * level, first, second


def exchange(
    sizes, loader_owner, slab_order, sectioned, out, kept, scales, peaks, sums, arrive, ld, pick, snd, own, stage,
    coded, tops, mine, ours, got, met, slots, origin, ls, s1, r1, s2, r2, sa, ra, sm, rm, so, ro,
):
    owners, tp, slab_rows, rows, pieces, per_block, columns, ahead, loads, sends, codes = sizes
    t = lax.axis_index("tp")
    f = lax.axis_index("fsdp")
    width = columns // pieces
    tiles = width // LANES
    chunks = slab_rows // rows * pieces

    def row_span(c):
        return pl.ds(pl.multiple_of(c // pieces * rows, rows), rows)

    def column_span(c):
        return pl.ds(pl.multiple_of(lax.rem(c, pieces) * width, LANES), width)

    def load(c):
        slot = lax.rem(c, loads)
        return pltpu.make_async_copy(sectioned.at[:, row_span(c), column_span(c)], ld.at[slot], ls.at[slot])

    for c in range(min(loads, chunks)):
        load(c).start()

    barrier = pltpu.get_barrier_semaphore()
    for d in range(1, owners):
        pl.semaphore_signal(barrier, inc=1, device_id={"fsdp": lax.rem(f + d, owners)}, device_id_type=MESH)
    for e in range(1, tp):
        pl.semaphore_signal(barrier, inc=1, device_id={"tp": lax.rem(t + e, tp)}, device_id_type=MESH)

    def find_slot(d, _):
        to = lax.rem(f + d, owners)

        def look(p, found):
            s = (p // per_block * owners + to) * per_block + lax.rem(p, per_block)
            return jnp.where(loader_owner[s] == f, slab_order[s], found)

        slots[d] = lax.fori_loop(0, owners, look, 0)
        origin[d] = loader_owner[(d // per_block * owners + f) * per_block + lax.rem(d, per_block)]
        return 0

    lax.fori_loop(0, owners, find_slot, 0)
    mine[...] = jnp.zeros_like(mine)
    peaks[...] = jnp.zeros_like(peaks)
    tops[...] = jnp.zeros_like(tops)
    pl.semaphore_wait(barrier, owners - 1 + tp - 1)

    def first_hop(c, d):
        slot = lax.rem(c, sends)
        return pltpu.make_async_remote_copy(
            src_ref=snd.at[slot, d - 1],
            dst_ref=arrive.at[c, f],
            send_sem=s1.at[slot],
            recv_sem=r1.at[c],
            device_id={"fsdp": lax.rem(f + d, owners)},
            device_id_type=MESH,
        )

    def first_sent(slot):
        whole = snd.at[slot]
        pltpu.make_async_copy(whole, whole, s1.at[slot]).wait()

    def first_landed(c):
        whole = arrive.at[c, pl.ds(0, owners - 1)]
        pltpu.make_async_copy(whole, whole, r1.at[c]).wait()

    low = lax.broadcasted_iota(jnp.int32, (rows, LANES), 1) < BLOCK

    def push(c):
        load(c).wait()

        @pl.when(c >= sends)
        def _():
            first_sent(lax.rem(c, sends))

        def take(o, _):
            pick[o] = ld[lax.rem(c, loads), o]
            return 0

        lax.fori_loop(0, owners, take, 0)

        @pl.when(c + loads < chunks)
        def _():
            load(c + loads).start()

        def choose(d, _):
            snd[lax.rem(c, sends), d - 1] = pick[slots[d]]
            return 0

        lax.fori_loop(1, owners, choose, 0)
        own[lax.rem(c, sends)] = pick[slots[0]]
        for d in order(owners):
            first_hop(c, d).start()

        def add(o, _):
            w = jnp.abs(pick[o].astype(jnp.float32))
            total = jnp.zeros((rows, LANES), jnp.float32)
            for j in range(tiles):
                top = w[:, j * LANES : (j + 1) * LANES]
                first = jnp.max(jnp.where(low, top, 0.0), axis=1, keepdims=True)
                second = jnp.max(jnp.where(low, 0.0, top), axis=1, keepdims=True)
                total = total + jnp.broadcast_to(first + second, total.shape)
            mine[...] += total
            return 0

        lax.fori_loop(0, owners, add, 0)

    def second_hop(c, e):
        slot = lax.rem(c, codes)
        return pltpu.make_async_remote_copy(
            src_ref=coded.at[slot, e - 1],
            dst_ref=out.at[e - 1, :, row_span(c), column_span(c)],
            send_sem=s2.at[slot],
            recv_sem=r2.at[c],
            device_id={"tp": lax.rem(t + e, tp)},
            device_id_type=MESH,
        )

    def second_sent(slot):
        whole = coded.at[slot]
        pltpu.make_async_copy(whole, whole, s2.at[slot]).wait()

    def second_landed(c):
        whole = coded.at[0]
        pltpu.make_async_copy(whole, whole, r2.at[c]).wait()

    def top_hop(r, e):
        span = pl.ds(pl.multiple_of(r * rows, rows), rows)
        return pltpu.make_async_remote_copy(
            src_ref=tops.at[e - 1, :, span],
            dst_ref=scales.at[e - 1, :, span],
            send_sem=sa.at[r],
            recv_sem=ra.at[r],
            device_id={"tp": lax.rem(t + e, tp)},
            device_id_type=MESH,
        )

    def top_done(r, sem):
        span = pl.ds(pl.multiple_of(r * rows, rows), rows)
        whole = tops.at[:, :, span]
        pltpu.make_async_copy(whole, whole, sem.at[r]).wait()

    def code(c, e):
        lane = lax.broadcasted_iota(jnp.int32, (rows, LANES), 1)
        to = lax.rem(t + e, tp)
        start = lax.rem(c, pieces) * (2 * tiles)

        def place(k, _):
            w = stage[origin[to * per_block + k]].astype(jnp.float32)
            if e < tp:
                held = tops[e - 1, k, row_span(c), :]
            else:
                held = peaks[k, row_span(c), :]
            made = []
            for j in range(tiles):
                value, first, second = code_tile(w[:, j * LANES : (j + 1) * LANES])
                made.append(value.astype(jnp.bfloat16))
                index = start + 2 * j
                held = jnp.where(lane == index, first, jnp.where(lane == index + 1, second, held))
            made = jnp.concatenate(made, axis=1)
            if e < tp:
                coded[lax.rem(c, codes), e - 1, k] = made
                tops[e - 1, k, row_span(c), :] = held
            else:
                kept[k, row_span(c), column_span(c)] = made
                peaks[k, row_span(c), :] = held
            return 0

        lax.fori_loop(0, per_block, place, 0)

    def sum_hop(d):
        return pltpu.make_async_remote_copy(
            src_ref=mine,
            dst_ref=got.at[d],
            send_sem=sm.at[d],
            recv_sem=rm.at[d],
            device_id={"fsdp": lax.rem(f + d, owners)},
            device_id_type=MESH,
        )

    def sum_turn(e):
        return pltpu.make_async_remote_copy(
            src_ref=ours,
            dst_ref=met.at[e],
            send_sem=so.at[e],
            recv_sem=ro.at[e],
            device_id={"tp": lax.rem(t + e, tp)},
            device_id_type=MESH,
        )

    def start_sums():
        for d in range(1, owners):
            sum_hop(d).start()

    def prime(c, _):
        push(c)
        return 0

    lax.fori_loop(0, ahead, prime, 0)
    if ahead == chunks:
        start_sums()

    def chunk(c, _):
        @pl.when(c + ahead < chunks)
        def _():
            push(c + ahead)

        if ahead < chunks:

            @pl.when(c + ahead == chunks - 1)
            def _():
                start_sums()

        first_landed(c)

        def take(d, _):
            o = lax.rem(f + d, owners)
            stage[o] = arrive[c, o]
            return 0

        lax.fori_loop(1, owners, take, 0)
        stage[f] = own[lax.rem(c, sends)]

        @pl.when(c >= codes)
        def _():
            second_sent(lax.rem(c, codes))

        for e in range(1, tp + 1):
            code(c, e)
            if e < tp:
                second_hop(c, e).start()

        @pl.when(lax.rem(c, pieces) == pieces - 1)
        def _():
            for e in range(1, tp):
                top_hop(c // pieces, e).start()

        return 0

    lax.fori_loop(0, chunks, chunk, 0)

    for d in range(1, owners):
        sum_hop(d).wait()
    total = mine[...]
    for d in range(1, owners):
        total = total + got[d]
    ours[...] = total
    for e in range(1, tp):
        sum_turn(e).start()
    for c in range(max(chunks - sends, 0), chunks):
        first_sent(c % sends)
    for c in range(max(chunks - codes, 0), chunks):
        second_sent(c % codes)

    def settle_tops(r, _):
        top_done(r, sa)
        top_done(r, ra)
        return 0

    lax.fori_loop(0, chunks // pieces, settle_tops, 0)

    def finish(c, _):
        second_landed(c)
        return 0

    lax.fori_loop(0, chunks, finish, 0)
    for e in range(1, tp):
        sum_turn(e).wait()
    total = ours[...]
    for e in range(1, tp):
        total = total + met[e]
    sums[...] = total


def order(owners):
    middle = owners // 2
    return sorted(range(1, owners), key=lambda d: (abs(d - middle), d))


def place_out(sizes, coded, kept, scales, peaks, sums, out, codes_out, tops_out, codes, spread, table, peak_lines, sem, sent):
    blocks, entries, count = sizes
    per_block, slab_rows, width = kept.shape
    tp = table.shape[0]
    me = lax.axis_index("tp")
    group = 256
    copies = []
    for e in range(tp):
        t = lax.rem(me + tp - e, tp)
        band = out.at[:, :, pl.ds(pl.multiple_of(t * width, LANES), width)]
        whole = coded.at[e - 1] if e else kept
        for k in range(per_block):
            copies.append(pltpu.make_async_copy(whole.at[k], band.at[k], sem.at[e, k]))
            copies[-1].start()
    for e in range(tp):
        table[lax.rem(me + tp - e, tp)] = scales[e - 1] if e else peaks[...]

    step = math.gcd(entries, group)
    period, turns = group // step, entries // step
    height = per_block * slab_rows // period
    lane = lax.broadcasted_iota(jnp.int32, (height, LANES), 1)
    offset = jnp.sum(sums[...], axis=0, keepdims=True) / count

    columns = [None] * (2 * turns)

    def lay(at, value):
        columns[at] = value if columns[at] is None else columns[at] + value

    def emit(j):
        left = columns[2 * j] - offset
        right = columns[2 * j + 1] - offset
        largest = jnp.maximum(jnp.abs(left), jnp.abs(right))
        largest = jnp.broadcast_to(jnp.max(largest, axis=1, keepdims=True), left.shape)
        scale = largest + EPS
        rows = pl.ds(j, height, stride=turns)
        codes[0, rows, :] = left / scale
        codes[1, rows, :] = right / scale
        spread[rows, :] = largest

    done = 0
    for i in range(period):
        for t in range(tp):
            piece = table[t, pl.ds(i, height, stride=period), :]
            at, shift = divmod(i * entries + t * blocks, LANES)
            if shift:
                piece = pltpu.roll(piece, shift, 1)
                lay(at, jnp.where(lane >= shift, piece, 0.0))
                if shift + blocks > LANES:
                    lay(at + 1, jnp.where(lane < shift, piece, 0.0))
            else:
                lay(at, piece)
            filled = (i * entries + (t + 1) * blocks) // group
            while done < filled:
                emit(done)
                done += 1

    row = lax.broadcasted_iota(jnp.int32, (LANES, LANES), 0)
    diagonal = row == lax.broadcasted_iota(jnp.int32, (LANES, LANES), 1)
    total = codes.shape[1]
    for s in range(total // LANES + (total % LANES > 0)):
        size = min(LANES, total - s * LANES)
        part = jnp.where(diagonal[:size], spread[s * LANES : s * LANES + size, :], 0.0)
        peak_lines[s : s + 1, :] = jnp.sum(part, axis=0, keepdims=True)
    copies.append(pltpu.make_async_copy(peak_lines, tops_out, sent.at[2]))
    copies[-1].start()
    for h in range(2):
        copies.append(pltpu.make_async_copy(codes.at[h], codes_out.at[:, pl.ds(h * LANES, LANES)], sent.at[h]))
        copies[-1].start()
    for copy in copies:
        copy.wait()


def per_device(sectioned, loader_owner, slab_order):
    owners = lax.axis_size("fsdp")
    tp = lax.axis_size("tp")
    slots, slab_rows, columns = sectioned.shape
    slab_count = loader_owner.shape[0]
    per_block = owners // tp
    rows = min(16, slab_rows)
    groups = columns // LANES
    pieces = next(p for p in (4, 2, 1) if groups % p == 0)
    width = columns // pieces
    chunks = slab_rows // rows * pieces
    ahead = min(3, chunks)
    loads, sends, codes = 2, min(ahead + 2, chunks), min(3, chunks)
    blocks = columns // BLOCK
    sizes = (owners, tp, slab_rows, rows, pieces, per_block, columns, ahead, loads, sends, codes)
    dma = pltpu.SemaphoreType.DMA
    anywhere = pl.BlockSpec(memory_space=pl.ANY)
    vmem = pl.BlockSpec(memory_space=pltpu.VMEM)
    smem = pl.BlockSpec(memory_space=pltpu.SMEM)
    half, full = jnp.bfloat16, jnp.float32
    buffers = [
        ((chunks, owners, rows, width), half),
        ((loads, owners, rows, width), half),
        ((owners, rows, width), half),
        ((sends, owners - 1, rows, width), half),
        ((sends, rows, width), half),
        ((owners, rows, width), half),
        ((codes, tp - 1, per_block, rows, width), half),
        ((tp - 1, per_block, slab_rows, LANES), full),
        ((rows, LANES), full),
        ((rows, LANES), full),
        ((owners, rows, LANES), full),
        ((tp, rows, LANES), full),
    ]
    held = sum(int(np.prod(shape)) * jnp.dtype(kind).itemsize for shape, kind in buffers)
    coded, kept, scales, peaks, sums = pl.pallas_call(
        functools.partial(exchange, sizes),
        out_shape=(
            pltpu.VMEM((tp - 1, per_block, slab_rows, columns), half),
            pltpu.VMEM((per_block, slab_rows, columns), half),
            pltpu.VMEM((tp - 1, per_block, slab_rows, LANES), full),
            pltpu.VMEM((per_block, slab_rows, LANES), full),
            pltpu.VMEM((rows, LANES), full),
        ),
        in_specs=[smem, smem, anywhere],
        out_specs=(vmem,) * 5,
        scratch_shapes=[pltpu.VMEM(shape, kind) for shape, kind in buffers]
        + [
            pltpu.SMEM((owners,), jnp.int32),
            pltpu.SMEM((owners,), jnp.int32),
            dma((loads,)),
            dma((sends,)),
            dma((chunks,)),
            dma((codes,)),
            dma((chunks,)),
            dma((chunks // pieces,)),
            dma((chunks // pieces,)),
            dma((owners,)),
            dma((owners,)),
            dma((tp,)),
            dma((tp,)),
        ],
        compiler_params=pltpu.CompilerParams(
            collective_id=0, has_side_effects=True, vmem_limit_bytes=held + 3 * 2**19
        ),
        name="exchange",
    )(loader_owner, slab_order, sectioned)
    entries = tp * blocks
    total = per_block * slab_rows * entries // 256
    lines = -(-total // LANES)
    dequant, scale_codes, tops = pl.pallas_call(
        functools.partial(place_out, (blocks, entries, float(slab_count * slab_rows * entries))),
        out_shape=(
            jax.ShapeDtypeStruct((per_block, slab_rows, tp * columns), half),
            jax.ShapeDtypeStruct((total, 2 * LANES), full),
            jax.ShapeDtypeStruct((lines, LANES), full),
        ),
        in_specs=[vmem] * 5,
        out_specs=(anywhere,) * 3,
        scratch_shapes=[
            pltpu.VMEM((2, total, LANES), full),
            pltpu.VMEM((total, LANES), full),
            pltpu.VMEM((tp, per_block * slab_rows, LANES), full),
            pltpu.VMEM((lines, LANES), full),
            dma((tp, per_block)),
            dma((3,)),
        ],
        compiler_params=pltpu.CompilerParams(vmem_limit_bytes=7 * 2**19),
        name="place_out",
    )(coded, kept, scales.reshape(tp - 1, -1, LANES), peaks.reshape(-1, LANES), sums)
    dequant = dequant.reshape(per_block * slab_rows, tp * columns)
    return (dequant, scale_codes, tops.reshape(-1)[:total])


def solution(mesh):
    return jax.shard_map(
        per_device,
        mesh=mesh,
        in_specs=(P("fsdp", None, "tp"), P(), P()),
        out_specs=(P(("tp", "fsdp"), None), P(("tp", "fsdp"), None), P(("tp", "fsdp"))),
        check_vma=False,
    )
```
